256 devices in a mesh: order: 16 (over z, core), blk: 16 (over x, y).
Axes of the slice: x: 4, y: 4, z: 8, core: 2. Of those that a mesh axis runs over, the one named last changes fastest.
Arguments:
- latent: bfloat16 [2, 16, 2048, 2048], P(None, None, 'order', 'blk'), may hold values from -0.1875 to 0.1875
- legendre: bfloat16 [2048, 2048, 256], P('order', 'blk'), may hold values from -0.125 to 0.125
- counts: int32 [256, 16, 4096], P(('blk', 'order')), may hold values from 0 to 7
- exposure: float32 [256, 4096], P(('blk', 'order')), may hold values from 0.25 to 4
- slot_order: int32 [2048], replicated, may hold values from 0 to 2047, each once
Outputs:
- gradient: float32 [2, 16, 2048, 2048], P(None, None, 'order', 'blk')
The draws below stay inside these ranges and needn't reach their ends.
Inputs may be any that keep to these rules, and one draw needn't show every extreme that they name: Slot s holds order slot_order[s]; every order from 0 to 2047 is held by exactly one slot.
All inputs are finite; a program needn't handle non-finite values.
Results may differ from the reference program's by a relative error of at most 0.005.
Values may be sent and summed in bfloat16 or wider, within the bound.
A program may use at most 64 MiB of HBM per device.

```python
import math
import jax
import jax.numpy as jnp
from jax import lax

L = 2048
NLON = 4096
CH = 16
CYCLES = 256


def touch_ends(values, key, least, high):
    longest = values.shape.index(max(values.shape))
    spots = []
    for shift in (0, 1):
        where = [jax.random.randint(jax.random.fold_in(key, axis), (), 0, length) for axis, length in enumerate(values.shape)]
        where[longest] = (where[longest] + shift) % values.shape[longest]
        spots.append(tuple(where))
    return values.at[spots[0]].set(least).at[spots[1]].set(high)


def levels(stream_key, extent, shards, low, top_value):
    gain = 1.0
    for dim, parts in shards:
        heights = jax.random.uniform(jax.random.fold_in(jax.random.fold_in(stream_key, 6), dim), (parts,), jnp.float32, low / len(shards), top_value / len(shards))
        gain = gain * jnp.repeat(jnp.exp(heights), extent[dim] // parts).reshape((-1,) + (1,) * (len(extent) - 1 - dim))
    return gain


def normal_values(rng, shape, width, bound, shards=(), kind=jnp.bfloat16):
    drawn = jax.random.normal(rng, shape, jnp.float32) * width
    if len(shards) > 0:
        drawn = levels(rng, shape, shards, -0.22, 0.18) * drawn
    return jnp.clip(drawn, min=-bound, max=bound).astype(kind)


def setup_inputs(seed: int = 0) -> dict:
    keys = jax.random.split(jax.random.key(seed), 6)
    return {
        "latent": normal_values(keys[0], (2, CH, L, L), (0.8 * (2 * L) ** -0.5), 0.1875, ((2, 16), (3, 16))),
        "legendre": normal_values(keys[1], (L, L, CYCLES), L ** -0.5, 0.125, ((0, 16), (1, 16))),
        "counts": touch_ends(jax.random.randint(keys[2], (CYCLES, CH, NLON), 0, 8), jax.random.fold_in(keys[2], 1), 0, 7).astype(jnp.int32),
        "exposure": jnp.clip(jnp.exp(math.log(4.0) - 2.7725887 * jax.random.uniform(keys[3], (CYCLES, NLON), jnp.float32) ** levels(keys[3], (CYCLES, NLON), ((0, 256),), -0.2, 0.2)), 0.25, 4.0),
        "slot_order": jax.random.permutation(keys[4], L).astype(jnp.int32),
    }


def reference(latent, legendre, counts, exposure, slot_order):
    degree = jnp.arange(L, dtype=jnp.int32)
    nonzero = degree[None, :] >= slot_order[:, None]
    masked = jnp.where(nonzero[None, None], latent, jnp.zeros((), latent.dtype))
    group_size = min(128, L)
    groups = L // group_size
    tables = legendre.reshape(groups, group_size, L, CYCLES)
    coefficients = jnp.moveaxis(masked, 2, 0).reshape(groups, group_size, 2, CH, L)

    def forward(operands):
        basis, values = operands
        return jnp.einsum('spcl,slr->rpcs', values.astype(jnp.float32), basis.astype(jnp.float32), precision=lax.Precision.HIGHEST)
    spectra = lax.map(forward, (tables, coefficients))
    spectra = jnp.moveaxis(spectra, 0, 3).reshape(CYCLES, 2, CH, L).astype(jnp.bfloat16)
    weight = jnp.where(slot_order == 0, 1.0, 2.0).astype(jnp.float32)
    scaled = spectra.astype(jnp.float32) * weight
    spectrum = jnp.zeros((CYCLES, 2, CH, NLON), jnp.float32).at[:, :, :, slot_order].set(scaled)
    latent_map = (jnp.fft.ifft(spectrum[:, 0] + 1j * spectrum[:, 1], axis=-1).real * NLON).astype(jnp.float32)
    cycle_index = jnp.arange(CYCLES, dtype=jnp.float32)
    cycle_area = jnp.sin(jnp.pi * (cycle_index + 0.5) / CYCLES)
    weight_map = cycle_area[:, None] * exposure
    growth = weight_map[:, None, :] * jnp.exp(latent_map)
    total_growth = lax.optimization_barrier(jnp.sum(growth, axis=(0, 2)))
    observed = counts.astype(jnp.float32)
    total_counts = lax.optimization_barrier(jnp.sum(observed, axis=(0, 2)))
    intensity = growth * (total_counts / total_growth)[None, :, None]
    residual = ((intensity - observed) * (1.0 / math.sqrt(NLON))).astype(jnp.bfloat16)
    transform = jnp.fft.fft(residual.astype(jnp.float32), axis=-1)
    picked = transform[:, :, slot_order]
    returned = (jnp.stack([picked.real, picked.imag], axis=1).astype(jnp.float32) * weight).astype(jnp.bfloat16)
    returns = jnp.moveaxis(returned.reshape(CYCLES, 2, CH, groups, group_size), 3, 0)

    def adjoint(operands):
        basis, values = operands
        return jnp.einsum('rpcs,slr->pcsl', values.astype(jnp.float32), basis.astype(jnp.float32), precision=lax.Precision.HIGHEST)
    gradients = lax.map(adjoint, (tables, returns))
    gradient = jnp.moveaxis(gradients, 0, 2).reshape(2, CH, L, L)
    return jnp.where(nonzero[None, None], gradient, jnp.zeros((), jnp.float32))
```

```python
import functools
import math

import jax
import jax.numpy as jnp
import numpy as np
from jax import lax
from jax.experimental import pallas as pl
from jax.experimental.pallas import tpu as pltpu
from jax.sharding import Mesh
from jax.sharding import PartitionSpec as P

BLK = ("blk_0", "blk_1")
ORDER = ("order_0", "order_1")
BLK_ORDER = ("blk_0", "blk_1", "order_0", "order_1")
AXES = ("order_0", "order_1", "blk_0", "blk_1")
MESH = pl.DeviceIdType.MESH
F32 = jnp.float32
BF16 = jnp.bfloat16

GROUP = 16


def hi_lo(x):
    hi = x.astype(BF16)
    return hi, (x - hi.astype(F32)).astype(BF16)


def dot(a, b):
    return jnp.dot(a, b, preferred_element_type=F32)


def np_hi_lo(x):
    x = np.asarray(x, np.float32)
    hi = x.astype(jnp.bfloat16)
    lo = (x - hi.astype(np.float32)).astype(jnp.bfloat16)
    return hi, lo


@functools.cache
def tables():
    a = np.arange(64)
    b = np.arange(32)
    j0 = np.arange(32)
    j1 = np.arange(128)
    turn = 2.0 * np.pi
    aj = turn * ((a[:, None] * j1[None, :]) % 128) / 128.0
    bj0 = turn * ((b[:, None] * j0[None, :]) % 32) / 32.0
    bj1 = turn * ((b[:, None] * j1[None, :]) % 4096) / 4096.0
    first = np.zeros((2, 64, 2, 2, 128))
    last = np.zeros((2, 2, 128, 2, 2, 64))
    for b2 in range(2):
        first[b2, :, b2, 0] = np.cos(aj)
        first[b2, :, b2, 1] = np.sin(aj)
        last[b2, 0, :, 0, b2] = np.cos(aj).T
        last[b2, 1, :, 0, b2] = np.sin(aj).T
        last[b2, 0, :, 1, b2] = -np.sin(aj).T
        last[b2, 1, :, 1, b2] = np.cos(aj).T
    fh, fl = np_hi_lo(first.reshape(128, 512))
    t1 = np.concatenate([fh, fl], axis=0)
    lh, ll = np_hi_lo(last.reshape(512, 256))
    t4 = np.concatenate([lh, ll], axis=0)
    w3 = np.concatenate([np.cos(bj0).T, -np.sin(bj0).T], axis=1)
    wh, wl = np_hi_lo(w3)
    w3 = np.concatenate([wh, wl, wh], axis=1)
    b_of = np.array([2 * b1 + b2 for b2 in range(2) for b1 in range(16)])
    v = np.concatenate([np.cos(bj0)[b_of], -np.sin(bj0)[b_of]], axis=0)
    vh, vl = np_hi_lo(v)
    w3b = np.concatenate([vh, vl, vh], axis=1)
    tw = np.concatenate([np.cos(bj1), np.sin(bj1)], axis=0).astype(np.float32)
    twb = np.concatenate([np.cos(bj1)[b_of], np.sin(bj1)[b_of]], axis=0).astype(np.float32)
    return t1, t4, w3, w3b, tw, twb


def spectra_kernel(lat_ref, leg_ref, out_ref, acc):
    g = pl.program_id(0)
    for i in range(GROUP):
        res = dot(lat_ref[i], leg_ref[i])
        row = g * GROUP + i
        acc[0, pl.ds(row, 32, stride=128), :] = res[:, :128]
        acc[1, pl.ds(row, 32, stride=128), :] = res[:, 128:]

    @pl.when(g == pl.num_programs(0) - 1)
    def _():
        def step(pc, _):
            for t in range(2):
                tile = acc[t, pl.ds(pl.multiple_of(pc * 128, 128), 128), :].T.astype(BF16)
                for q in range(8):
                    e = 8 * t + q
                    out_ref[e // 4, e % 4, pc] = tile[16 * q : 16 * q + 16]
            return 0

        lax.fori_loop(0, 32, step, 0)


def partial_spectra(lat, leg):
    return pl.pallas_call(
        spectra_kernel,
        grid=(128 // GROUP,),
        out_shape=jax.ShapeDtypeStruct((4, 4, 32, 16, 128), BF16),
        in_specs=[
            pl.BlockSpec((GROUP, 32, 128), lambda g: (g, 0, 0)),
            pl.BlockSpec((GROUP, 128, 256), lambda g: (g, 0, 0)),
        ],
        out_specs=pl.BlockSpec((4, 4, 32, 16, 128), lambda g: (0, 0, 0, 0, 0)),
        scratch_shapes=[pltpu.VMEM((2, 4096, 128), F32)],
        compiler_params=pltpu.CompilerParams(vmem_limit_bytes=40 * 2**20),
    )(lat, leg)


def gradient_kernel(first_degree_ref, order_ref, ret_ref, leg_ref, out_ref, acc):
    g = pl.program_id(0)

    @pl.when(g == 0)
    def _():
        def step(pc, _):
            for t in range(2):
                rows = [ret_ref[(8 * t + q) // 4, (8 * t + q) % 4, pc] for q in range(8)]
                tile = jnp.concatenate(rows, axis=0).astype(F32).T
                acc[t, pl.ds(pl.multiple_of(pc * 128, 128), 128), :] = tile
            return 0

        lax.fori_loop(0, 32, step, 0)

    degree = first_degree_ref[0] + lax.broadcasted_iota(jnp.int32, (1, 128), 1)
    for i in range(GROUP):
        row = g * GROUP + i
        lhs = jnp.concatenate(
            [acc[t, pl.ds(row, 32, stride=128), :] for t in range(2)], axis=1
        ).astype(BF16)
        res = lax.dot_general(
            lhs, leg_ref[i], (((1,), (1,)), ((), ())), preferred_element_type=F32
        )
        out_ref[pl.ds(i, 32, stride=GROUP), :] = jnp.where(degree >= order_ref[row], res, 0.0)


def latent_gradient(first_degree, orders_here, ret, leg):
    return pl.pallas_call(
        gradient_kernel,
        grid_spec=pltpu.PrefetchScalarGridSpec(
            num_scalar_prefetch=2,
            grid=(128 // GROUP,),
            in_specs=[
                pl.BlockSpec((4, 4, 32, 16, 128), lambda g, *_: (0, 0, 0, 0, 0)),
                pl.BlockSpec((GROUP, 128, 256), lambda g, *_: (g, 0, 0)),
            ],
            out_specs=pl.BlockSpec((None, 32 * GROUP, 128), lambda g, *_: (g, 0, 0)),
            scratch_shapes=[pltpu.VMEM((2, 4096, 128), F32)],
        ),
        out_shape=jax.ShapeDtypeStruct((128 // GROUP, 32 * GROUP, 128), F32),
        compiler_params=pltpu.CompilerParams(vmem_limit_bytes=40 * 2**20),
    )(first_degree, orders_here, ret, leg)


def sky_kernel(
    part, counts, weight, order_cols, t1, t4, w3, w3b, tw, twb, ret,
    in1, direct1, fwd_src, fwd1, y1, land2, spec_f, spec_b, spec_in,
    oh, oht, a1, zs, zb, xb, vb, ug, uc, un, rb, rr, fb, ga, tot_src, tot_in, tot2_src, tot2_in,
    send_sem, recv_sem,
):
    z, core = lax.axis_index("order_0"), lax.axis_index("order_1")
    x, y = lax.axis_index("blk_0"), lax.axis_index("blk_1")
    k = z * 2 + core
    b = x * 4 + y

    def order_peer(i):
        other = lax.rem(k + i, 16)
        return other, (other // 2, lax.rem(other, 2), x, y)

    def blk_peer(i):
        other = lax.rem(b + i, 16)
        return other, (z, core, other // 4, lax.rem(other, 4))

    def ring(h, i):
        if h == 0:
            return (z, core, lax.rem(x + i + 4, 4), y)
        return (z, core, x, lax.rem(y + i + 4, 4))

    barrier = pltpu.get_barrier_semaphore()
    for i in range(1, 16):
        pl.semaphore_signal(barrier, inc=1, device_id=order_peer(i)[1], device_id_type=MESH)
        pl.semaphore_signal(barrier, inc=1, device_id=blk_peer(i)[1], device_id_type=MESH)
    pl.semaphore_wait(barrier, 30)

    used = [0]
    started = []

    def send(src, dst, device):
        n = used[0]
        used[0] += 1
        copy = pltpu.make_async_remote_copy(
            src_ref=src,
            dst_ref=dst,
            send_sem=send_sem.at[n],
            recv_sem=recv_sem.at[n],
            device_id=device,
            device_id_type=MESH,
        )
        copy.start()
        started.append(copy)
        return copy

    def at(h, d, half):
        d = lax.rem(d + 4, 4)
        if h == 0:
            return part.at[d, pl.ds(2 * half, 2), pl.ds(0, 16)]
        return part.at[pl.ds(2 * half, 2), d, pl.ds(16, 16)]

    def load(h, d, half, row, pc):
        d = lax.rem(d + 4, 4)
        if h == 0:
            return part[d, 2 * half + row, pc].astype(F32)
        return part[2 * half + row, d, 16 + pc].astype(F32)

    q = (x, y)
    near, straight = {}, {}
    for h in range(2):
        for s, sign in enumerate((1, -1)):
            near[h, s] = send(at(h, q[h] + 2, s), in1.at[h, s], ring(h, sign))
    for h in range(2):
        for s, sign in enumerate((1, -1)):
            straight[h, s] = send(at(h, q[h] + sign, 1 - s), direct1.at[h, s], ring(h, sign))

    lane = lax.broadcasted_iota(jnp.int32, (128, 128), 1)
    sub = lax.broadcasted_iota(jnp.int32, (128, 128), 0)

    def build(i, _):
        cols = jnp.broadcast_to(order_cols[pl.ds(i, 1), :], (128, 128))
        rows = cols.T
        for t in range(16):
            value = 2.0
            value_t = 2.0
            if t == 0:
                value = jnp.where(lane == 0, 1.0, 2.0)
                value_t = jnp.where(sub == 0, 1.0, 2.0)
            base = 128 * t
            oh[i, :, 128 * t : 128 * t + 128] = jnp.where(rows == lane + base, value, 0.0).astype(BF16)
            oht[t, i] = jnp.where(cols == sub + base, value_t, 0.0).astype(BF16)
        return 0

    def relay(h, s, sign):
        near[h, s].wait_recv()

        def add(pc, _):
            for row in range(2):
                total = in1[h, s, row, pc].astype(F32) + load(h, q[h] + sign, s, row, pc)
                fwd_src[h, s, row, pc] = total.astype(BF16)
            return 0

        lax.fori_loop(0, 16, add, 0)
        return send(fwd_src.at[h, s], fwd1.at[h, s], ring(h, sign))

    def to_orders(out):
        for c in range(0, 16, 2):
            pair = jnp.concatenate(
                [xb[pl.ds(c + e, 32, stride=16), :] for e in range(2)], axis=1
            )
            ph, plo = hi_lo(pair)
            v = dot(w3b[...], jnp.concatenate([ph, ph, plo], axis=0))
            for e in range(2):
                re, im = v[:32, 128 * e : 128 * e + 128], v[32:, 128 * e : 128 * e + 128]
                co, si = twb[0:32, :], twb[32:64, :]
                turned = (re * co + im * si, im * co - re * si)
                for b2 in range(2):
                    for ri in range(2):
                        vb[2 * b2 + ri, pl.ds(c + e, 16, stride=16), :] = turned[ri][
                            16 * b2 : 16 * b2 + 16
                        ]
        lhs = jnp.concatenate([vb[i] for i in range(4)], axis=1)
        lh, ll = hi_lo(lhs)
        out[...] = dot(lh, t4[0:512, :]) + dot(lh, t4[512:1024, :]) + dot(ll, t4[0:512, :])

    count_sum = jnp.zeros((16, 128), F32)
    for j in range(32):
        tile = counts[:, 128 * j : 128 * j + 128].astype(F32)
        xb[16 * j : 16 * j + 16, :] = tile
        count_sum = count_sum + tile
    to_orders(uc)

    passed = {}
    for h in range(2):
        for s, sign in enumerate((1, -1)):
            passed[h, s] = relay(h, s, sign)

    lax.fori_loop(0, 16, build, 0)

    second = {}
    for h in range(2):
        for s in range(2):
            straight[h, s].wait_recv()
            passed[h, s].wait_recv()

        def add(pc, _):
            for half in range(2):
                for row in range(2):
                    total = (
                        load(h, q[h], half, row, pc)
                        + fwd1[h, half, row, pc].astype(F32)
                        + direct1[h, 1 - half, row, pc].astype(F32)
                    )
                    y1[h, 2 * half + row, pc] = total.astype(BF16)
            return 0

        lax.fori_loop(0, 16, add, 0)
        for i in range(1, 4):
            d = lax.rem(q[1 - h] + i, 4)
            second[h, i] = send(y1.at[h, d], land2.at[h, i - 1], ring(1 - h, i))
    for h in range(2):
        for i in range(1, 4):
            second[h, i].wait_recv()

        def add(pc, _):
            total = y1[h, q[1 - h], pc].astype(F32)
            for i in range(3):
                total = total + land2[h, i, pc].astype(F32)
            spec_f[pl.ds(16 * h + pc, 16, stride=32), :] = total
            return 0

        lax.fori_loop(0, 16, add, 0)
    spec_b[...] = spec_f[...].astype(BF16).reshape(16, 32, 128)

    moved = {}
    for i in range(1, 16):
        other, device = order_peer(i)
        moved[i] = send(spec_b.at[other], spec_in.at[k], device)
    spec_in[k] = spec_b[k]
    for i in range(1, 16):
        moved[i].wait_recv()

    lhs = jnp.concatenate([spec_in[i] for i in range(16)], axis=1)
    for t in range(8):
        rhs = jnp.concatenate([oh[i, :, 256 * t : 256 * t + 256] for i in range(16)], axis=0)
        tile = dot(lhs, rhs).astype(BF16)
        for e in range(2):
            a1[32 * (2 * t + e) : 32 * (2 * t + e) + 32, :] = tile[:, 128 * e : 128 * e + 128]
    twice = jnp.concatenate([a1[...], a1[...]], axis=1)
    zs[...] = dot(twice, t1[...])
    for b1 in range(16):
        for b2 in range(2):
            bb = 2 * b1 + b2
            top, bottom = 32 * b1, 32 * b1 + 16
            c0 = zs[top : top + 16, 256 * b2 : 256 * b2 + 128]
            d0 = zs[top : top + 16, 256 * b2 + 128 : 256 * b2 + 256]
            c1 = zs[bottom : bottom + 16, 256 * b2 : 256 * b2 + 128]
            d1 = zs[bottom : bottom + 16, 256 * b2 + 128 : 256 * b2 + 256]
            re, im = c0 - d1, d0 + c1
            co, si = tw[bb : bb + 1, :], tw[32 + bb : 33 + bb, :]
            zb[pl.ds(bb, 16, stride=64), :] = re * co - im * si
            zb[pl.ds(32 + bb, 16, stride=64), :] = re * si + im * co
    for c in range(0, 16, 2):
        pair = jnp.concatenate([zb[64 * (c + e) : 64 * (c + e) + 64, :] for e in range(2)], axis=1)
        ph, plo = hi_lo(pair)
        m = dot(w3[...], jnp.concatenate([ph, ph, plo], axis=0))
        for e in range(2):
            xb[pl.ds(c + e, 32, stride=16), :] = m[:, 128 * e : 128 * e + 128]
    growth_sum = jnp.zeros((16, 128), F32)
    for j in range(32):
        tile = weight[:, 128 * j : 128 * j + 128] * jnp.exp(xb[16 * j : 16 * j + 16, :])
        xb[16 * j : 16 * j + 16, :] = tile
        growth_sum = growth_sum + tile

    chain = lax.broadcasted_iota(jnp.int32, (16, 128), 0)
    lane16 = lax.broadcasted_iota(jnp.int32, (16, 128), 1)
    row = jnp.where(lane16 == chain, jnp.sum(growth_sum, axis=1, keepdims=True), 0.0) + jnp.where(
        lane16 == chain + 16, jnp.sum(count_sum, axis=1, keepdims=True), 0.0
    )
    row = jnp.sum(row, axis=0, keepdims=True)
    tot_src[...] = jnp.broadcast_to(row, (8, 128))
    sums = {}
    for i in range(1, 16):
        sums[i] = send(tot_src, tot_in.at[i - 1], order_peer(i)[1])
    to_orders(ug)
    total = tot_src[...]
    for i in range(1, 16):
        sums[i].wait_recv()
        total = total + tot_in[i - 1]
    tot2_src[...] = total
    for i in range(1, 16):
        sums[i] = send(tot2_src, tot2_in.at[i - 1], blk_peer(i)[1])
    for i in range(1, 16):
        sums[i].wait_recv()
        total = total + tot2_in[i - 1]
    row = jnp.broadcast_to(total[0:1, :], (16, 128))
    total_growth = jnp.sum(jnp.where(lane16 == chain, row, 0.0), axis=1, keepdims=True)
    total_counts = jnp.sum(jnp.where(lane16 == chain + 16, row, 0.0), axis=1, keepdims=True)
    ratio = jnp.broadcast_to(total_counts / total_growth, (16, 256))

    for b1 in range(16):
        rows = slice(16 * b1, 16 * b1 + 16)
        u = (ug[rows, :] * ratio - uc[rows, :]) * (1.0 / 64.0)
        un[:, 128 * b1 : 128 * b1 + 128] = jnp.concatenate([u[:, :128], u[:, 128:]], axis=0).astype(BF16)
    for i in range(0, 16, 2):
        rhs = jnp.concatenate(
            [jnp.concatenate([oht[t, i + e] for t in range(16)], axis=0) for e in range(2)], axis=1
        )
        r = dot(un[...], rhs).astype(BF16)
        for e in range(2):
            rb[i + e] = r[:, 128 * e : 128 * e + 128]
    for i in range(1, 16):
        other, device = order_peer(i)
        moved[i] = send(rb.at[other], rr.at[k], device)
    rr[k] = rb[k]
    for i in range(1, 16):
        moved[i].wait_recv()
    for i in range(16):
        fb[pl.ds(i, 32, stride=16), :] = rr[i].astype(F32)
    ga[x, y] = fb[...].astype(BF16).reshape(32, 16, 128)

    def own(h):
        return ga.at[x, y, pl.ds(16 * h, 16)]

    first = {}
    for h in range(2):
        for i in range(1, 4):
            first[h, i] = send(own(h), own(h), ring(1 - h, i))

    def group(h, d, half):
        d = lax.rem(d + 4, 4)
        if h == 0:
            return ga.at[d, pl.ds(2 * half, 2), pl.ds(0, 16)]
        return ga.at[pl.ds(2 * half, 2), d, pl.ds(16, 16)]

    for h in range(2):
        for i in range(1, 4):
            first[h, i].wait_recv()
        for s, sign in enumerate((1, -1)):
            near[h, s] = send(group(h, q[h], s), group(h, q[h], s), ring(h, sign))
        for s, sign in enumerate((1, -1)):
            straight[h, s] = send(group(h, q[h], 1 - s), group(h, q[h], 1 - s), ring(h, sign))
    for h in range(2):
        for s, sign in enumerate((1, -1)):
            near[h, s].wait_recv()
            piece = group(h, q[h] - sign, s)
            passed[h, s] = send(piece, piece, ring(h, sign))
    for h in range(2):
        for s in range(2):
            straight[h, s].wait_recv()
            passed[h, s].wait_recv()
    for copy in started:
        copy.wait_send()
    ret[...] = ga[...]


N_SENDS = 12 + 6 + 15 + 30 + 15 + 6 + 12


def sky(part, counts, weight, order_cols):
    t = [jnp.asarray(a) for a in tables()]
    vm = pltpu.VMEM
    return pl.pallas_call(
        sky_kernel,
        out_shape=jax.ShapeDtypeStruct((4, 4, 32, 16, 128), BF16),
        in_specs=[pl.BlockSpec(memory_space=pltpu.VMEM)] * (4 + len(t)),
        out_specs=pl.BlockSpec(memory_space=pltpu.VMEM),
        scratch_shapes=[
            vm((2, 2, 2, 16, 16, 128), BF16),
            vm((2, 2, 2, 16, 16, 128), BF16),
            vm((2, 2, 2, 16, 16, 128), BF16),
            vm((2, 2, 2, 16, 16, 128), BF16),
            vm((2, 4, 16, 16, 128), BF16),
            vm((2, 3, 16, 16, 128), BF16),
            vm((512, 128), F32),
            vm((16, 32, 128), BF16),
            vm((16, 32, 128), BF16),
            vm((16, 128, 2048), BF16),
            vm((16, 16, 128, 128), BF16),
            vm((512, 128), BF16),
            vm((512, 512), F32),
            vm((1024, 128), F32),
            vm((512, 128), F32),
            vm((4, 256, 128), F32),
            vm((256, 256), F32),
            vm((256, 256), F32),
            vm((32, 2048), BF16),
            vm((16, 32, 128), BF16),
            vm((16, 32, 128), BF16),
            vm((512, 128), F32),
            vm((4, 4, 32, 16, 128), BF16),
            vm((8, 128), F32),
            vm((15, 8, 128), F32),
            vm((8, 128), F32),
            vm((15, 8, 128), F32),
            pltpu.SemaphoreType.DMA((N_SENDS,)),
            pltpu.SemaphoreType.DMA((N_SENDS,)),
        ],
        compiler_params=pltpu.CompilerParams(
            collective_id=0, has_side_effects=True, vmem_limit_bytes=58 * 2**20
        ),
    )(part, counts, weight, order_cols, *t)


def body(latent, legendre, counts, exposure, slot_order):
    slot_count, degrees, cycle_count = legendre.shape
    orders_here = lax.dynamic_slice_in_dim(
        slot_order, lax.axis_index(ORDER) * slot_count, slot_count
    )
    first_degree = lax.axis_index(BLK) * degrees
    degree = first_degree + lax.iota(jnp.int32, degrees)
    nonzero = degree[None, :] >= orders_here[:, None]
    masked = jnp.where(nonzero[None, None], latent, jnp.zeros((), latent.dtype))
    lat = jnp.transpose(masked.reshape(32, slot_count, degrees), (1, 0, 2))
    part = partial_spectra(lat, legendre)
    cycle = lax.axis_index(BLK) * lax.axis_size(ORDER) + lax.axis_index(ORDER)
    cycle_area = jnp.sin(jnp.pi * (cycle.astype(F32) + 0.5) / 256)
    weight = cycle_area * exposure
    order_cols = (lax.rem(slot_order, 32) * 64 + slot_order // 32).reshape(16, 128)
    ret = sky(part, counts[0], weight, order_cols)
    grad = latent_gradient(first_degree[None], orders_here, ret, legendre)
    grad = grad.reshape(128 // GROUP, 32, GROUP, 128).transpose(1, 0, 2, 3)
    return grad.reshape(2, 16, slot_count, degrees)


def solution(mesh):
    finer = Mesh(mesh.devices.reshape(8, 2, 4, 4), AXES)
    return jax.shard_map(
        body,
        mesh=finer,
        in_specs=(
            P(None, None, ORDER, BLK),
            P(ORDER, BLK, None),
            P(BLK_ORDER, None, None),
            P(BLK_ORDER, None),
            P(),
        ),
        out_specs=P(None, None, ORDER, BLK),
        check_vma=False,
    )
```
